256 devices in a mesh: batch: 16 (over y, z_lo), mp: 16 (over z_hi, x, core).
Axes of the slice: x: 4, y: 4, z: 8 (z_hi: 2, z_lo: 4; z = z_hi * 4 + z_lo), core: 2. Of those that a mesh axis runs over, the one named last changes fastest.
Arguments:
- gate_act: bfloat16 [12288, 14336], P('batch', 'mp'), may hold values from -6 to 6
- up_act: bfloat16 [12288, 14336], P('batch', 'mp'), may hold values from -6 to 6
- upstream: bfloat16 [12288, 8192], P('batch', 'mp'), may hold values from -6 to 6
- kept_index: int32 [16, 16], P('batch'), may hold values from 0 to 31, as said below
- kept_count: int32 [16], P('batch'), may hold values from 1 to 16, as said below
Outputs:
- grad_down: bfloat16 [8192, 14336], P('batch', 'mp')
The draws below stay inside these ranges and needn't reach their ends.
Inputs may be any that keep to these rules, and one draw needn't show every extreme that they name: `kept_index`: each group's row names different candidates; only the first kept_count entries of a row are kept. `kept_count`: the counts sum to 16 * 8 over the groups, and some group keeps exactly 16.
All inputs are finite; a program needn't handle non-finite values.
Results may differ from the reference program's by a relative error of at most 0.0049.
Values may be sent and summed in bfloat16 or wider, within the bound.
No kernel may reach another device: no remote copies, remote signals or barrier semaphores. Data moves between devices by JAX's collectives and lax.ppermute only.
A program may use at most 128 MiB of HBM per device.

```python
import math
import jax
import jax.numpy as jnp
from jax import lax

D = 8192
FF_W = 14336
SEQ = 24
CAND = 32
GROUPS = 16
KEEP_MAX = 16
CAP = 8
N_BATCH = 16


def draw_kept_count(key, part):
    first_key, second_key = jax.random.split(jax.random.fold_in(key, 11))
    biggest = jax.random.randint(first_key, (), 0, GROUPS)
    counts = jnp.ones((GROUPS,), jnp.int32).at[biggest].set(KEEP_MAX)
    extra = GROUPS * CAP - KEEP_MAX - (GROUPS - 1)
    places = jnp.arange(GROUPS, dtype=jnp.int32)

    def add_one(step, counts):
        anchor = jax.random.randint(jax.random.fold_in(second_key, step), (), 0, GROUPS)
        distance = jnp.mod(places - anchor, GROUPS)
        score = jnp.where(counts < KEEP_MAX, GROUPS - distance, 0)
        target = jnp.argmax(score)
        return counts + (places == target).astype(jnp.int32)
    return lax.fori_loop(0, extra, add_one, counts)


def draw_kept_index(key, part):
    row_keys = jax.random.split(jax.random.fold_in(key, 23), GROUPS)

    def one_row(row_key):
        return jax.random.permutation(row_key, CAND)[:KEEP_MAX].astype(jnp.int32)
    return jax.vmap(one_row)(row_keys)


def spiked(values, own_key, source, target, blocks, factor):
    owner, partner = [(jnp.arange(values.shape[position]) // (values.shape[position] // blocks)).reshape([-1 if axis == position else 1 for axis in range(values.ndim)]) for position in (source, target)]
    chosen = jax.random.permutation(own_key, blocks)[partner]
    strong = (owner == chosen) | (owner == (partner + blocks // 2) % blocks)
    return jnp.where(strong, factor * values, values)


def levels(own_key, dims, cuts, smallest, largest):
    gain = 1.0
    for dim, shards_of in cuts:
        steps = jax.random.uniform(jax.random.fold_in(jax.random.fold_in(own_key, 6), dim), (shards_of,), jnp.float32, smallest / len(cuts), largest / len(cuts))
        gain = gain * jnp.repeat(jnp.exp(steps), dims[dim] // shards_of).reshape((-1,) + (1,) * (len(dims) - 1 - dim))
    return gain


def bell_draw(own_key, extent, spread, reach, cuts=(), kind=jnp.bfloat16):
    result = jax.random.normal(own_key, extent, jnp.float32) * spread
    if len(cuts) > 0:
        result = levels(own_key, extent, cuts, -0.22, 0.18) * result
    return jnp.clip(result, min=-reach, max=reach).astype(kind)


def heavy_noise(stream_key, shape, spread, bound, cuts, heavy, kind=jnp.bfloat16):
    result = spread * jax.random.normal(stream_key, shape, jnp.float32)
    if cuts:
        result = result * levels(stream_key, shape, cuts, -0.22, 0.18)
    return jnp.clip(spiked(result, jax.random.fold_in(stream_key, 3), *heavy), -bound, bound).astype(kind)


def setup_inputs(seed: int = 0) -> dict:
    arg_keys = jax.random.split(jax.random.key(seed), 6)
    gate_act = bell_draw(arg_keys[0], (N_BATCH * CAND * SEQ, FF_W), 1.0, 6.0, ((0, 16), (1, 16)))
    up_act = bell_draw(arg_keys[1], (N_BATCH * CAND * SEQ, FF_W), 1.0, 6.0, ((0, 16), (1, 16)))
    upstream = heavy_noise(arg_keys[2], (N_BATCH * CAND * SEQ, D), 1.0, 6.0, ((0, 16), (1, 16)), (0, 1, 16, 2.0))
    kept_index = draw_kept_index(jax.random.fold_in(arg_keys[5], 71), 0)
    kept_count = draw_kept_count(jax.random.fold_in(arg_keys[5], 71), 0)
    return dict(gate_act=gate_act, up_act=up_act, upstream=upstream, kept_index=kept_index, kept_count=kept_count)


def reference(gate_act, up_act, upstream, kept_index, kept_count):
    gate_all = gate_act.reshape(N_BATCH, CAND, SEQ, FF_W)
    up_all = up_act.reshape(N_BATCH, CAND, SEQ, FF_W)
    grad_all = upstream.reshape(N_BATCH, CAND, SEQ, D)
    slot_ids = jnp.arange(KEEP_MAX, dtype=jnp.int32)

    def per_group(summed, group_id):
        picked = kept_index[group_id]
        present = slot_ids < kept_count[group_id]
        gate_rows = gate_all[group_id][picked].astype(jnp.float32)
        up_rows = up_all[group_id][picked].astype(jnp.float32)
        hidden = (jax.nn.silu(gate_rows) * up_rows).astype(jnp.bfloat16)
        hidden = jnp.where(present[:, None, None], hidden, jnp.zeros_like(hidden))
        grad_rows = grad_all[group_id][picked]
        term = lax.dot_general(grad_rows.reshape(KEEP_MAX * SEQ, D), hidden.reshape(KEEP_MAX * SEQ, FF_W), (((0,), (0,)), ((), ())), preferred_element_type=jnp.float32)
        return (summed + term, None)
    summed, _ = lax.scan(per_group, jnp.zeros((D, FF_W), jnp.float32), jnp.arange(N_BATCH, dtype=jnp.int32))
    factor = 1.0 / math.sqrt(N_BATCH * CAP * SEQ)
    return (summed * factor).astype(jnp.bfloat16)
```

```python
import math

import jax
import jax.numpy as jnp
from jax import lax
from jax.sharding import Mesh
from jax.sharding import PartitionSpec as P

SEQ = 24
CAND = 32
CAP = 8
F_CUTS = (256, 384, 256)
E_CUTS = (256, 256)
SPREAD = ("zl", "zh", "x", "c")


def spread_pairs(sizes, flip):
    zl, zh, x, c = sizes

    def at(a, b, d, e):
        return ((a * zh + b) * x + d) * c + e

    pairs = []
    for z_from in range(zl):
        for h in range(zh):
            for i in range(x):
                for k in range(c):
                    z_to = (i % 2) * 2 + k
                    r = z_to ^ z_from
                    pairs.append((at(z_from, h, i, k), at(z_to, h ^ flip, (i // 2) * 2 + r // 2, r % 2)))
    return pairs


def swap(value, axis, bit):
    n = lax.axis_size(axis)
    return lax.ppermute(value, axis, [(i, i ^ bit) for i in range(n)])


def along_z(part):
    near = swap(part, "zl", 1)
    far = swap(part, "zl", 2)
    middle = lax.ppermute(part, "zl", [(1, 2), (2, 1)])
    passed = lax.ppermute(far, "zl", [(2, 3), (1, 0)])
    z = lax.axis_index("zl")
    last = jnp.where((z == 1) | (z == 2), middle, passed)
    return jnp.stack([part, near, far, last])


def on_device(gate_act, up_act, upstream, kept_index, kept_count):
    slots = kept_index.shape[1]
    rows = slots * SEQ
    hidden_width = gate_act.shape[1]
    model_part = upstream.shape[1]
    picked = kept_index[0]
    present = jnp.arange(slots, dtype=jnp.int32) < kept_count[0]
    y, z, zh, x, c = (lax.axis_index(a) for a in ("y", "zl", "zh", "x", "c"))

    grads = upstream.reshape(CAND, SEQ, model_part)[picked].reshape(rows, model_part).T
    grad_parts, at = [], 0
    sizes = tuple(lax.axis_size(a) for a in SPREAD)
    for width in E_CUTS:
        mine = grads[at : at + width]
        at += width
        own = jnp.stack([lax.ppermute(mine, SPREAD, spread_pairs(sizes, k)) for k in (0, 1)])
        by_x = [own] + [swap(own, "x", s) for s in (1, 2, 3)]
        by_c = [[p, swap(p, "c", 1)] for p in by_x]
        blocks = []
        for k in (0, 1):
            for high in (0, 1):
                blocks.append(
                    jnp.concatenate([by_c[2 * high + low][o][k] for low in (0, 1) for o in (0, 1)], axis=1)
                )
        grad_parts.append(jnp.concatenate(blocks, axis=0))

    gate_all = gate_act.reshape(CAND, SEQ, hidden_width)
    up_all = up_act.reshape(CAND, SEQ, hidden_width)
    hidden = (
        jax.nn.silu(gate_all[picked].astype(jnp.float32)) * up_all[picked].astype(jnp.float32)
    ).astype(jnp.bfloat16)
    hidden = jnp.where(present[:, None, None], hidden, jnp.zeros_like(hidden)).reshape(rows, hidden_width)
    offset = 2 * (x % 2) + c
    order = jnp.bitwise_xor(jnp.arange(4, dtype=jnp.int32), offset)
    hidden_parts, at = [], 0
    for width in F_CUTS:
        got = along_z(hidden[:, at : at + width])
        at += width
        hidden_parts.append(got[order].reshape(4 * rows, width))

    first = ((y // 2) ^ zh) * 2 + ((y % 2) ^ (x // 2))
    factor = 1.0 / math.sqrt(lax.axis_size("y") * lax.axis_size("zl") * CAP * SEQ)
    columns = []
    for h in hidden_parts:
        pieces = []
        for g in grad_parts:
            partial = jnp.dot(g, h, preferred_element_type=jnp.float32).astype(jnp.bfloat16)
            partial = partial.reshape(4, -1, h.shape[1])
            total = lax.dynamic_index_in_dim(partial, first, 0, keepdims=False).astype(jnp.float32)
            for d in (1, 2, 3):
                out = lax.dynamic_index_in_dim(partial, first ^ d, 0, keepdims=False)
                total = total + swap(out, "y", d).astype(jnp.float32)
            pieces.append((total * factor).astype(jnp.bfloat16))
        columns.append(jnp.concatenate(pieces, axis=0))
    return jnp.concatenate(columns, axis=1)


def solution(mesh):
    split = Mesh(mesh.devices.reshape(4, 4, 2, 4, 2), ("y", "zl", "zh", "x", "c"))
    batch, mp = ("y", "zl"), ("zh", "x", "c")
    in_specs = (P(batch, mp), P(batch, mp), P(batch, mp), P(batch, None), P(batch))
    return jax.shard_map(
        on_device, mesh=split, in_specs=in_specs, out_specs=P(batch, mp), check_vma=False
    )
```

```python
import math

import jax
import jax.numpy as jnp
from jax import lax
from jax.experimental import pallas as pl
from jax.experimental.pallas import tpu as pltpu
from jax.sharding import Mesh
from jax.sharding import PartitionSpec as P


SEQ = 24
CAND = 32
CAP = 8
F_CUTS = (512, 384)
E_CUTS = (256, 256)
SPREAD = ("zl", "zh", "x", "c")
SMEM = pl.BlockSpec(memory_space=pltpu.SMEM)
VMEM = pl.BlockSpec(memory_space=pltpu.VMEM)


def spread_pairs(sizes, flip):
    zl, zh, x, c = sizes

    def at(a, b, d, e):
        return ((a * zh + b) * x + d) * c + e

    pairs = []
    for z_from in range(zl):
        for h in range(zh):
            for i in range(x):
                for k in range(c):
                    z_to = (i % 2) * 2 + k
                    r = z_to ^ z_from
                    pairs.append((at(z_from, h, i, k), at(z_to, h ^ flip, (i // 2) * 2 + r // 2, r % 2)))
    return pairs


def swap(value, axis, bit):
    n = lax.axis_size(axis)
    return lax.ppermute(value, axis, [(i, i ^ bit) for i in range(n)])


def grads_body(rows, at_ref, own, rest, c_own, c_rest, out):
    width = own.shape[2]
    for s in range(4):
        for o in range(2):
            q = (s % 2) * 2 + o
            for k in range(2):
                d = (k * 2 + s // 2) ^ at_ref[0]
                source = (own, c_own)[o].at[k] if s == 0 else (rest, c_rest)[o].at[s - 1, k]
                columns = pl.ds(pl.multiple_of(d * width, 128), width)
                out[pl.ds(q * rows, rows), columns] = source[...]


def join_grads(first, own, rest, c_own, c_rest):
    rows, width = own.shape[1:]

    def body(*refs):
        grads_body(rows, *refs)

    return pl.pallas_call(
        body,
        out_shape=jax.ShapeDtypeStruct((4 * rows, 4 * width), own.dtype),
        in_specs=[SMEM, VMEM, VMEM, VMEM, VMEM],
        out_specs=VMEM,
        cost_estimate=pl.CostEstimate(flops=2_000_000_000, bytes_accessed=6_000_000, transcendentals=0),
    )(first, own, rest, c_own, c_rest)


def join_hidden(place, own, near, far, middle, passed):
    rows, width = own.shape

    def body(at_ref, own, near, far, middle, passed, out):
        def rows_of(r):
            return pl.ds(pl.multiple_of((r ^ at_ref[0]) * rows, rows), rows)

        out[rows_of(0), :] = own[...]
        out[rows_of(1), :] = near[...]
        out[rows_of(2), :] = far[...]

        @pl.when(at_ref[1] == 1)
        def _():
            out[rows_of(3), :] = middle[...]

        @pl.when(at_ref[1] == 0)
        def _():
            out[rows_of(3), :] = passed[...]

    return pl.pallas_call(
        body,
        out_shape=jax.ShapeDtypeStruct((4 * rows, width), own.dtype),
        in_specs=[SMEM, VMEM, VMEM, VMEM, VMEM, VMEM],
        out_specs=VMEM,
        cost_estimate=pl.CostEstimate(flops=1_000_000_000, bytes_accessed=3_000_000, transcendentals=0),
    )(place, own, near, far, middle, passed)


def on_device(gate_act, up_act, upstream, kept_index, kept_count):
    slots = kept_index.shape[1]
    rows = slots * SEQ
    hidden_width = gate_act.shape[1]
    model_part = upstream.shape[1]
    picked = kept_index[0]
    present = jnp.arange(slots, dtype=jnp.int32) < kept_count[0]
    y, z, zh, x, c = (lax.axis_index(a) for a in ("y", "zl", "zh", "x", "c"))
    sizes = tuple(lax.axis_size(a) for a in SPREAD)

    grads = upstream.reshape(CAND, SEQ, model_part)[picked].reshape(rows, model_part)
    owns, at = [], 0
    for width in E_CUTS:
        mine = grads[:, at : at + width]
        at += width
        got = []
        for k in (0, 1):
            got.append(lax.ppermute(mine, SPREAD, spread_pairs(sizes, k)))
        owns.append(jnp.stack(got))

    gate_all = gate_act.reshape(CAND, SEQ, hidden_width)
    up_all = up_act.reshape(CAND, SEQ, hidden_width)
    hidden = (
        jax.nn.silu(gate_all[picked].astype(jnp.float32)) * up_all[picked].astype(jnp.float32)
    ).astype(jnp.bfloat16)
    hidden = jnp.where(present[:, None, None], hidden, jnp.zeros_like(hidden)).reshape(rows, hidden_width)
    inner = ((z == 1) | (z == 2)).astype(jnp.int32)
    place = jnp.stack([(2 * (x % 2) + c).astype(jnp.int32), inner])
    hidden_parts, at = [], 0
    for width in F_CUTS:
        part = hidden[:, at : at + width]
        at += width
        far = swap(part, "zl", 2)
        near = swap(part, "zl", 1)
        middle = lax.ppermute(part, "zl", [(1, 2), (2, 1)])
        passed = lax.ppermute(far, "zl", [(2, 3), (1, 0)])
        hidden_parts.append(join_hidden(place, part, near, far, middle, passed))

    first = (((y // 2) ^ zh) * 2 + ((y % 2) ^ (x // 2))).astype(jnp.int32).reshape(1)
    grad_parts = []
    for own in owns:
        c_own = swap(own, "c", 1)
        rest = jnp.stack([swap(own, "x", s) for s in (1, 2, 3)])
        c_rest = swap(rest, "c", 1)
        grad_parts.append(join_grads(first, own, rest, c_own, c_rest))

    factor = 1.0 / math.sqrt(lax.axis_size("y") * lax.axis_size("zl") * CAP * SEQ)
    columns = []
    for h in hidden_parts:
        pieces = []
        for g in grad_parts:
            partial = lax.dot_general(
                g, h, (((0,), (0,)), ((), ())), preferred_element_type=jnp.float32
            ).astype(jnp.bfloat16)
            partial = partial.reshape(4, -1, h.shape[1])
            total = partial[0].astype(jnp.float32)
            for d in (1, 3, 2):
                total = total + swap(partial[d], "y", d).astype(jnp.float32)
            pieces.append((total * factor).astype(jnp.bfloat16))
        columns.append(jnp.concatenate(pieces, axis=0))
    return jnp.concatenate(columns, axis=1)


def solution(mesh):
    split = Mesh(mesh.devices.reshape(4, 4, 2, 4, 2), ("y", "zl", "zh", "x", "c"))
    batch, mp = ("y", "zl"), ("zh", "x", "c")
    in_specs = (P(batch, mp), P(batch, mp), P(batch, mp), P(batch, None), P(batch))

    return jax.shard_map(on_device, mesh=split, in_specs=in_specs, out_specs=P(batch, mp), check_vma=False)
```

```python
import math

import jax
import jax.numpy as jnp
from jax import lax
from jax.experimental import pallas as pl
from jax.experimental.pallas import tpu as pltpu
from jax.sharding import Mesh
from jax.sharding import PartitionSpec as P


SEQ = 24
CAND = 32
CAP = 8
F_CUTS = (512, 384)
SPREAD = ("zl", "zh", "x", "c")
SMEM = pl.BlockSpec(memory_space=pltpu.SMEM)
VMEM = pl.BlockSpec(memory_space=pltpu.VMEM)


def spread_pairs(sizes, flip):
    zl, zh, x, c = sizes

    def at(a, b, d, e):
        return ((a * zh + b) * x + d) * c + e

    pairs = []
    for z_from in range(zl):
        for h in range(zh):
            for i in range(x):
                for k in range(c):
                    z_to = (i % 2) * 2 + k
                    r = z_to ^ z_from
                    pairs.append((at(z_from, h, i, k), at(z_to, h ^ flip, (i // 2) * 2 + r // 2, r % 2)))
    return pairs


def swap(value, axis, bit):
    n = lax.axis_size(axis)
    return lax.ppermute(value, axis, [(i, i ^ bit) for i in range(n)])


def copy_rows(source, target, row):
    rows = source.shape[0]
    step = 128

    @pl.loop(0, rows // step)
    def _(i):
        target[pl.ds(row + i * step, step), :] = source[pl.ds(i * step, step), :]


def join_grads(first, parts):
    rows, width = parts[0][0][0].shape
    flat = [a for part in parts for pair in part for a in pair]
    kind = flat[0].dtype

    def body(at_ref, *refs):
        pieces, outs = refs[: len(flat)], refs[len(flat) :]
        for d in range(4):
            for block in range(4):

                @pl.when(block ^ at_ref[0] == d)
                def _(block=block, d=d):
                    k, high = block // 2, block % 2
                    for q in range(4):
                        copy_rows(pieces[k * 8 + (2 * high + q // 2) * 2 + q % 2], outs[d], q * rows)

    return pl.pallas_call(
        body,
        out_shape=[jax.ShapeDtypeStruct((4 * rows, width), kind)] * 4,
        in_specs=[SMEM] + [VMEM] * len(flat),
        out_specs=[VMEM] * 4,
        name="grads",
        compiler_params=pltpu.CompilerParams(vmem_limit_bytes=16 * 2**20),
        cost_estimate=pl.CostEstimate(flops=2_000_000_000, bytes_accessed=12_000_000, transcendentals=0),
    )(first, *flat)


def add_up(factor, done, own, got):
    rows, before = done.shape
    width = own.shape[1]

    def body(done, own, a, b, c, out):
        out[:, :before] = done[...]
        total = own[...] + a[...].astype(jnp.float32) + b[...].astype(jnp.float32) + c[...].astype(jnp.float32)
        out[:, before:] = (total * factor).astype(out.dtype)

    return pl.pallas_call(
        body,
        out_shape=jax.ShapeDtypeStruct((rows, before + width), done.dtype),
        in_specs=[VMEM] * 5,
        out_specs=VMEM,
        name="add",
        compiler_params=pltpu.CompilerParams(vmem_limit_bytes=8 * 2**20),
    )(done, own, *got)


def join_hidden(place, own, near, far, middle, passed):
    rows, width = own.shape

    def body(at_ref, own, near, far, middle, passed, out):
        def rows_of(r):
            return pl.ds(pl.multiple_of((r ^ at_ref[0]) * rows, rows), rows)

        out[rows_of(0), :] = own[...]
        out[rows_of(1), :] = near[...]
        out[rows_of(2), :] = far[...]

        @pl.when(at_ref[1] == 1)
        def _():
            out[rows_of(3), :] = middle[...]

        @pl.when(at_ref[1] == 0)
        def _():
            out[rows_of(3), :] = passed[...]

    return pl.pallas_call(
        body,
        out_shape=jax.ShapeDtypeStruct((4 * rows, width), own.dtype),
        in_specs=[SMEM, VMEM, VMEM, VMEM, VMEM, VMEM],
        out_specs=VMEM,
        compiler_params=pltpu.CompilerParams(vmem_limit_bytes=5 * 2**20),
        cost_estimate=pl.CostEstimate(flops=1_000_000_000, bytes_accessed=3_000_000, transcendentals=0),
    )(place, own, near, far, middle, passed)


def on_device(gate_act, up_act, upstream, kept_index, kept_count):
    slots = kept_index.shape[1]
    rows = slots * SEQ
    hidden_width = gate_act.shape[1]
    model_part = upstream.shape[1]
    picked = kept_index[0]
    present = jnp.arange(slots, dtype=jnp.int32) < kept_count[0]
    y, z, zh, x, c = (lax.axis_index(a) for a in ("y", "zl", "zh", "x", "c"))
    sizes = tuple(lax.axis_size(a) for a in SPREAD)

    grads = upstream.reshape(CAND, SEQ, model_part)[picked].reshape(rows, model_part)
    owns = []
    for k in (0, 1):
        owns.append(lax.ppermute(grads, SPREAD, spread_pairs(sizes, k)))

    gate_all = gate_act.reshape(CAND, SEQ, hidden_width)
    up_all = up_act.reshape(CAND, SEQ, hidden_width)
    hidden = (
        jax.nn.silu(gate_all[picked].astype(jnp.float32)) * up_all[picked].astype(jnp.float32)
    ).astype(jnp.bfloat16)
    hidden = jnp.where(present[:, None, None], hidden, jnp.zeros_like(hidden)).reshape(rows, hidden_width)
    inner = ((z == 1) | (z == 2)).astype(jnp.int32)
    place = jnp.stack([(2 * (x % 2) + c).astype(jnp.int32), inner])
    hidden_parts, at = [], 0
    for width in F_CUTS:
        part = hidden[:, at : at + width]
        at += width
        far = swap(part, "zl", 2)
        near = swap(part, "zl", 1)
        middle = lax.ppermute(part, "zl", [(1, 2), (2, 1)])
        passed = lax.ppermute(far, "zl", [(2, 3), (1, 0)])
        hidden_parts.append(join_hidden(place, part, near, far, middle, passed))

    first = (((y // 2) ^ zh) * 2 + ((y % 2) ^ (x // 2))).astype(jnp.int32).reshape(1)
    parts = []
    for own in owns:
        by_x = [own] + [swap(own, "x", s) for s in (1, 2, 3)]
        parts.append([(a, swap(a, "c", 1)) for a in by_x])
    blocks = join_grads(first, parts)

    factor = 1.0 / math.sqrt(lax.axis_size("y") * lax.axis_size("zl") * CAP * SEQ)
    dims = (((0,), (0,)), ((), ()))
    sums = []
    for h in hidden_parts:
        got = []
        for d in (1, 3, 2, 0):
            partial = lax.dot_general(blocks[d], h, dims, preferred_element_type=jnp.float32)
            if d:
                partial = partial.astype(jnp.bfloat16)
            got.append(swap(partial, "y", d) if d else partial)
        sums.append((got[3], got[:3]))
    own, got = sums[0]
    done = (own + got[0].astype(jnp.float32) + got[1].astype(jnp.float32) + got[2].astype(jnp.float32)) * factor
    return add_up(factor, done.astype(jnp.bfloat16), *sums[1])


def solution(mesh):
    split = Mesh(mesh.devices.reshape(4, 4, 2, 4, 2), ("y", "zl", "zh", "x", "c"))
    batch, mp = ("y", "zl"), ("zh", "x", "c")
    in_specs = (P(batch, mp), P(batch, mp), P(batch, mp), P(batch, None), P(batch))

    return jax.shard_map(on_device, mesh=split, in_specs=in_specs, out_specs=P(batch, mp), check_vma=False)
```

```python
import math

import jax
import jax.numpy as jnp
from jax import lax
from jax.experimental import pallas as pl
from jax.experimental.pallas import tpu as pltpu
from jax.sharding import Mesh
from jax.sharding import PartitionSpec as P


SEQ = 24
CAND = 32
CAP = 8
F_CUTS = (512, 384)
SPREAD = ("zl", "zh", "x", "c")
SMEM = pl.BlockSpec(memory_space=pltpu.SMEM)
VMEM = pl.BlockSpec(memory_space=pltpu.VMEM)


def spread_pairs(sizes, flip, moved):
    zl, zh, x, c = sizes

    def at(a, b, d, e):
        return ((a * zh + b) * x + d) * c + e

    pairs = []
    for z_from in range(zl):
        for h in range(zh):
            for i in range(x):
                for k in range(c):
                    z_to = ((i ^ moved) % 2) * 2 + k
                    r = z_to ^ z_from
                    pairs.append((at(z_from, h, i, k), at(z_to, h ^ flip, (i // 2) * 2 + r // 2, r % 2)))
    return pairs


def swap(value, axis, bit):
    n = lax.axis_size(axis)
    return lax.ppermute(value, axis, [(i, i ^ bit) for i in range(n)])


def copy_rows(source, target, row):
    rows = source.shape[0]
    step = 192

    @pl.loop(0, rows // step)
    def _(i):
        target[pl.ds(row + i * step, step), :] = source[pl.ds(i * step, step), :]


def join_grads(first, parts):
    rows, width = parts[0][0][0].shape[1:]
    flat = [a for part in parts for pair in part for a in pair]
    kind = flat[0].dtype
    whole = rows * len(parts)

    def body(at_ref, *refs):
        pieces, outs = refs[: len(flat)], refs[len(flat) :]
        for d in range(4):
            for block in range(4):

                @pl.when(block ^ at_ref[0] == d)
                def _(block=block, d=d):
                    k, high = block // 2, block % 2
                    for h in range(len(parts)):
                        for q in range(4):
                            piece = pieces[h * 8 + (2 * high + q // 2) * 2 + q % 2]
                            copy_rows(piece.at[k], outs[d], q * whole + h * rows)

    return pl.pallas_call(
        body,
        out_shape=[jax.ShapeDtypeStruct((4 * whole, width), kind)] * 4,
        in_specs=[SMEM] + [VMEM] * len(flat),
        out_specs=[VMEM] * 4,
        name="grads",
        compiler_params=pltpu.CompilerParams(vmem_limit_bytes=16 * 2**20),
        cost_estimate=pl.CostEstimate(flops=2_000_000_000, bytes_accessed=12_000_000, transcendentals=0),
    )(first, *flat)


def add_up(factor, done, own, got):
    rows, before = done.shape
    width = own.shape[1]

    def body(done, own, a, b, c, out):
        out[:, :before] = done[...]
        total = own[...] + a[...].astype(jnp.float32) + b[...].astype(jnp.float32) + c[...].astype(jnp.float32)
        out[:, before:] = (total * factor).astype(out.dtype)

    return pl.pallas_call(
        body,
        out_shape=jax.ShapeDtypeStruct((rows, before + width), done.dtype),
        in_specs=[VMEM] * 5,
        out_specs=VMEM,
        name="add",
        compiler_params=pltpu.CompilerParams(vmem_limit_bytes=8 * 2**20),
    )(done, own, *got)


def join_hidden(place, own, near, far, middle, passed):
    rows, width = own.shape

    def body(at_ref, own, near, far, middle, passed, out):
        def rows_of(r):
            return pl.ds(pl.multiple_of((r ^ at_ref[0]) * rows, rows), rows)

        out[rows_of(0), :] = own[...]
        out[rows_of(1), :] = near[...]
        out[rows_of(2), :] = far[...]

        @pl.when(at_ref[1] == 1)
        def _():
            out[rows_of(3), :] = middle[...]

        @pl.when(at_ref[1] == 0)
        def _():
            out[rows_of(3), :] = passed[...]

    return pl.pallas_call(
        body,
        out_shape=jax.ShapeDtypeStruct((4 * rows, width), own.dtype),
        in_specs=[SMEM, VMEM, VMEM, VMEM, VMEM, VMEM],
        out_specs=VMEM,
        compiler_params=pltpu.CompilerParams(vmem_limit_bytes=5 * 2**20),
        cost_estimate=pl.CostEstimate(flops=1_000_000_000, bytes_accessed=3_000_000, transcendentals=0),
    )(place, own, near, far, middle, passed)


def on_device(gate_act, up_act, upstream, kept_index, kept_count):
    slots = kept_index.shape[1]
    rows = slots * SEQ
    hidden_width = gate_act.shape[1]
    model_part = upstream.shape[1]
    picked = kept_index[0]
    present = jnp.arange(slots, dtype=jnp.int32) < kept_count[0]
    y, z, zh, x, c = (lax.axis_index(a) for a in ("y", "zl", "zh", "x", "c"))
    sizes = tuple(lax.axis_size(a) for a in SPREAD)

    grads = upstream.reshape(CAND, SEQ, model_part)[picked].reshape(rows, model_part)
    half = rows // 2
    owns = []
    for h, mine in enumerate((grads[:half], swap(grads[half:], "x", 1))):
        got = []
        for k in (0, 1):
            got.append(lax.ppermute(mine, SPREAD, spread_pairs(sizes, k, h)))
        owns.append(jnp.stack(got))

    gate_all = gate_act.reshape(CAND, SEQ, hidden_width)
    up_all = up_act.reshape(CAND, SEQ, hidden_width)
    hidden = (
        jax.nn.silu(gate_all[picked].astype(jnp.float32)) * up_all[picked].astype(jnp.float32)
    ).astype(jnp.bfloat16)
    hidden = jnp.where(present[:, None, None], hidden, jnp.zeros_like(hidden)).reshape(rows, hidden_width)
    inner = ((z == 1) | (z == 2)).astype(jnp.int32)
    place = jnp.stack([(2 * (x % 2) + c).astype(jnp.int32), inner])
    hidden_parts, at = [], 0
    for width in F_CUTS:
        part = hidden[:, at : at + width]
        at += width
        far = swap(part, "zl", 2)
        near = swap(part, "zl", 1)
        middle = lax.ppermute(part, "zl", [(1, 2), (2, 1)])
        passed = lax.ppermute(far, "zl", [(2, 3), (1, 0)])
        hidden_parts.append(join_hidden(place, part, near, far, middle, passed))

    first = (((y // 2) ^ zh) * 2 + ((y % 2) ^ (x // 2))).astype(jnp.int32).reshape(1)
    parts = []
    for own in owns:
        one, three = (swap(own, "x", s) for s in (1, 3))
        two = jnp.stack([swap(one[0], "x", 3), swap(three[1], "x", 1)])
        by_x = [own, one, two, three]
        parts.append([(a, swap(a, "c", 1)) for a in by_x])
    blocks = join_grads(first, parts)

    factor = 1.0 / math.sqrt(lax.axis_size("y") * lax.axis_size("zl") * CAP * SEQ)
    dims = (((0,), (0,)), ((), ()))
    sums = []
    for h in hidden_parts:
        got = []
        for d in (2, 1, 3, 0):
            partial = lax.dot_general(blocks[d], h, dims, preferred_element_type=jnp.float32)
            if d:
                partial = partial.astype(jnp.bfloat16)
            got.append(swap(partial, "y", d) if d else partial)
        sums.append((got[3], got[:3]))
    own, got = sums[0]
    done = (own + got[0].astype(jnp.float32) + got[1].astype(jnp.float32) + got[2].astype(jnp.float32)) * factor
    return add_up(factor, done.astype(jnp.bfloat16), *sums[1])


def solution(mesh):
    split = Mesh(mesh.devices.reshape(4, 4, 2, 4, 2), ("y", "zl", "zh", "x", "c"))
    batch, mp = ("y", "zl"), ("zh", "x", "c")
    in_specs = (P(batch, mp), P(batch, mp), P(batch, mp), P(batch, None), P(batch))

    return jax.shard_map(on_device, mesh=split, in_specs=in_specs, out_specs=P(batch, mp), check_vma=False)
```
